32 devices in a mesh: dp: 4 (over y, x), tensor: 8 (over z, core).
Axes of the slice: x: 2, y: 2, z: 4, core: 2. Of those that a mesh axis runs over, the one named last changes fastest.
Arguments:
- tokens: bfloat16 [768, 4096], P(('dp', 'tensor')), may hold values from -6 to 6
- out_grad: bfloat16 [768, 4096], P(('dp', 'tensor')), may hold values from -6 to 6
- w_gate: bfloat16 [4096, 14336], P(None, 'tensor'), may hold values from -0.09375 to 0.09375
- w_up: bfloat16 [4096, 14336], P(None, 'tensor'), may hold values from -0.09375 to 0.09375
- w_down: bfloat16 [14336, 4096], P('tensor'), may hold values from -0.046875 to 0.046875
Outputs:
- grad_tokens: bfloat16 [768, 4096], P(('dp', 'tensor'))
- grad_gate: bfloat16 [4096, 14336], P('dp', 'tensor')
- grad_up: bfloat16 [4096, 14336], P('dp', 'tensor')
- grad_down: bfloat16 [14336, 4096], P('tensor', 'dp')
The draws below stay inside these ranges and needn't reach their ends.
All inputs are finite; a program needn't handle non-finite values.
Results may differ from the reference program's by a relative error of at most 0.014.
Values may be sent and summed in bfloat16 or wider, within the bound.
A program may use at most 128 MiB of HBM per device.

```python
import jax
import jax.numpy as jnp
from jax import lax

D = 4096
FF = 14336
TOKENS = 768
N_DP = 4


def block_scale(own_key, shape, shards, least, top_value):
    def one(position, shards_of):
        heights = jax.random.uniform(jax.random.fold_in(jax.random.fold_in(own_key, 6), position), (shards_of,), jnp.float32, least / len(shards), top_value / len(shards))
        return jnp.repeat(jnp.exp(heights), shape[position] // shards_of).reshape((-1,) + (1,) * (len(shape) - position - 1))

    level = one(*shards[0])
    for cut in shards[1:]:
        level = level * one(*cut)
    return level


def noise(key, dims, deviation, most, cuts=(), dtype=jnp.bfloat16):
    values = jax.random.normal(key, dims, jnp.float32) * deviation
    if len(cuts) > 0:
        values = block_scale(key, dims, cuts, -0.22, 0.18) * values
    return jnp.clip(values, min=-most, max=most).astype(dtype)


def setup_inputs(seed: int = 0) -> dict:
    key_list = jax.random.split(jax.random.key(seed), 6)
    tokens = noise(key_list[0], (TOKENS, D), 1.0, 6.0, ((0, 32),))
    out_grad = noise(key_list[1], (TOKENS, D), 1.0, 6.0, ((0, 32),))
    w_gate = noise(key_list[2], (D, FF), D ** -0.5, 0.09375, ((1, 8),))
    w_up = noise(key_list[3], (D, FF), D ** -0.5, 0.09375, ((1, 8),))
    w_down = noise(key_list[4], (FF, D), FF ** -0.5, 0.046875, ((0, 8),))
    return dict(tokens=tokens, out_grad=out_grad, w_gate=w_gate, w_up=w_up, w_down=w_down)


def reference(tokens, out_grad, w_gate, w_up, w_down):
    gate_val = jnp.dot(tokens, w_gate, preferred_element_type=jnp.float32)
    up_val = jnp.dot(tokens, w_up, preferred_element_type=jnp.float32)
    sigmoid_gate = jax.nn.sigmoid(gate_val)
    act_val = gate_val * sigmoid_gate
    hidden = (act_val * up_val).astype(jnp.bfloat16)
    grad_hidden = jnp.dot(out_grad, w_down.T, preferred_element_type=jnp.float32)
    grad_gate_pre = (grad_hidden * up_val * sigmoid_gate * (1.0 + gate_val * (1.0 - sigmoid_gate))).astype(jnp.bfloat16)
    grad_up_pre = (grad_hidden * act_val).astype(jnp.bfloat16)
    grad_tokens = (jnp.dot(grad_gate_pre, w_gate.T, preferred_element_type=jnp.float32)
                   + jnp.dot(grad_up_pre, w_up.T, preferred_element_type=jnp.float32)).astype(jnp.bfloat16)
    token_groups = tokens.reshape(N_DP, -1, D)
    grad_groups = out_grad.reshape(N_DP, -1, D)
    hidden_groups = hidden.reshape(N_DP, -1, FF)
    gate_groups = grad_gate_pre.reshape(N_DP, -1, FF)
    up_groups = grad_up_pre.reshape(N_DP, -1, FF)

    def rounded_add(total, left, right):
        partial_sum = jnp.dot(left.T, right, preferred_element_type=jnp.float32).astype(jnp.bfloat16)
        partial_sum = lax.optimization_barrier(partial_sum)
        return total + partial_sum.astype(jnp.float32)

    def one_group(carried, pieces):
        tok_g, grad_g, hid_g, gate_g, up_g = pieces
        sum_gate, sum_up, sum_down = carried
        return (rounded_add(sum_gate, tok_g, gate_g), rounded_add(sum_up, tok_g, up_g),
                rounded_add(sum_down, hid_g, grad_g)), None

    initial = (jnp.zeros((D, FF), jnp.float32), jnp.zeros((D, FF), jnp.float32), jnp.zeros((FF, D), jnp.float32))
    totals, unused = lax.scan(one_group, initial, (token_groups, grad_groups, hidden_groups, gate_groups, up_groups))
    return (grad_tokens, totals[0].astype(jnp.bfloat16), totals[1].astype(jnp.bfloat16),
            totals[2].astype(jnp.bfloat16))
```

```python
import functools

import jax
import jax.numpy as jnp
from jax import lax
from jax.experimental import pallas as pl
from jax.experimental.pallas import tpu as pltpu
from jax.sharding import PartitionSpec as P

MESH = pl.DeviceIdType.MESH


def lookup(index, table):
    value = jnp.int32(table[0])
    for k in range(1, len(table)):
        value = jnp.where(index == k, jnp.int32(table[k]), value)
    return value


def ring_order(n):
    return [p ^ (p >> 1) for p in range(n)] if n & (n - 1) == 0 else list(range(n))


def position(n_tensor):
    group, slot = lax.axis_index("dp"), lax.axis_index("tensor")
    return group, slot, slot // 2, slot % 2, n_tensor // 2


def gather_kernel(
    n_dp, n_tensor, tok, grad, out_tok, out_grad,
    line_send, line_recv, ring_send, ring_recv, pair_send, pair_recv, own_sem,
):
    group, slot, level, core, n_levels = position(n_tensor)
    order = ring_order(n_dp)
    where = {g: p for p, g in enumerate(order)}
    half = n_dp // 2

    def at_distance(s):
        return lookup(group, [order[(where[g] + s) % n_dp] for g in range(n_dp)])

    neighbours = (at_distance(1), at_distance(-1))
    origin = [[at_distance(-s) for s in range(half + 1)], [at_distance(s) for s in range(half + 1)]]
    partner = (group, level * 2 + 1 - core)
    ins, outs = (tok, grad), (out_tok, out_grad)

    def level_slot(k):
        return lax.rem(level + k + n_levels, n_levels) * 2 + core

    barrier = pltpu.get_barrier_semaphore()
    peers = [(group, level_slot(k)) for k in range(1, n_levels)]
    peers += [(neighbours[0], slot), (neighbours[1], slot), partner]
    for peer in peers:
        pl.semaphore_signal(barrier, inc=1, device_id=peer, device_id_type=MESH)
    pl.semaphore_wait(barrier, len(peers))

    started = []

    def send(src, dst, send_sem, recv_sem, peer):
        copy = pltpu.make_async_remote_copy(
            src_ref=src, dst_ref=dst, send_sem=send_sem, recv_sem=recv_sem,
            device_id=peer, device_id_type=MESH,
        )
        copy.start()
        started.append(copy)

    def arrived(ref, send_sem, recv_sem):
        pltpu.make_async_remote_copy(
            src_ref=ref, dst_ref=ref, send_sem=send_sem, recv_sem=recv_sem,
            device_id=partner, device_id_type=MESH,
        ).wait_recv()

    shared = []

    def share(src, ref, a, number):
        send(src, ref, pair_send.at[a, number], pair_recv.at[a, number], partner)

    def pair_slot(u):
        return lax.rem(level - u + n_levels, n_levels) * 2 + 1 - core

    def process_ring(u):
        spot = level_slot(-u)
        for s in range(1, half + 1):
            for direction in (0, 1):
                for a in (0, 1):
                    if s == half and a != direction:
                        continue
                    source = origin[direction][s]
                    ref = outs[a].at[source, spot]
                    arrived(ref, ring_send.at[u, s, direction, a], ring_recv.at[u, s, direction, a])
                    onward = s + 1
                    if onward < half or (onward == half and a == direction):
                        send(ref, ref, ring_send.at[u, onward, direction, a],
                             ring_recv.at[u, onward, direction, a], (neighbours[direction], slot))
                    number = u * n_dp + (s if direction == 0 else n_dp - s)
                    if s == half:
                        number = u * n_dp + half
                    share(ref, ref, a, number)
                    shared.append((a, number, source, pair_slot(u)))

    for direction in (0, 1):
        for a in (0, 1):
            if half > 1 or a == direction:
                send(ins[a], outs[a].at[group, slot], ring_send.at[0, 1, direction, a],
                     ring_recv.at[0, 1, direction, a], (neighbours[direction], slot))
    for k in range(1, n_levels):
        for a in (0, 1):
            send(ins[a], outs[a].at[group, slot], line_send.at[k, a], line_recv.at[k, a],
                 (group, level_slot(k)))
    own = []
    for a in (0, 1):
        share(ins[a], outs[a].at[group, slot], a, 0)
        shared.append((a, 0, group, pair_slot(0)))
        copy = pltpu.make_async_copy(ins[a], outs[a].at[group, slot], own_sem.at[a])
        copy.start()
        own.append(copy)

    for u in range(1, n_levels):
        process_ring(u - 1)
        spot = level_slot(-u)
        for a in (0, 1):
            ref = outs[a].at[group, spot]
            arrived(ref, line_send.at[u, a], line_recv.at[u, a])
            for direction in (0, 1):
                if half > 1 or a == direction:
                    send(ref, ref, ring_send.at[u, 1, direction, a],
                         ring_recv.at[u, 1, direction, a], (neighbours[direction], slot))
            share(ref, ref, a, u * n_dp)
            shared.append((a, u * n_dp, group, pair_slot(u)))
    process_ring(n_levels - 1)

    for a, number, source, spot in shared:
        arrived(outs[a].at[source, spot], pair_send.at[a, number], pair_recv.at[a, number])
    for copy in started:
        copy.wait_send()
    for copy in own:
        copy.wait()


def gather_tokens(tokens, out_grad, n_dp, n_tensor):
    rows, width = tokens.shape
    n_levels, half = n_tensor // 2, n_dp // 2
    full = jax.ShapeDtypeStruct((n_dp, n_tensor, rows, width), tokens.dtype)
    dma = pltpu.SemaphoreType.DMA
    anywhere = pl.BlockSpec(memory_space=pl.ANY)
    tok, grad = pl.pallas_call(
        functools.partial(gather_kernel, n_dp, n_tensor),
        out_shape=(full, full),
        in_specs=[anywhere] * 2,
        out_specs=(anywhere, anywhere),
        scratch_shapes=[
            dma((n_levels, 2)), dma((n_levels, 2)),
            dma((n_levels, half + 1, 2, 2)), dma((n_levels, half + 1, 2, 2)),
            dma((2, n_levels * n_dp)), dma((2, n_levels * n_dp)),
            dma((2,)),
        ],
        compiler_params=pltpu.CompilerParams(collective_id=0, has_side_effects=True),
        name="gather_tokens",
    )(tokens, out_grad)
    return tok.reshape(-1, width), grad.reshape(-1, width)


def scatter_kernel(
    n_tensor, part, out, mine, theirs, summed, landed,
    mine_sem, pair_send, pair_recv, line_send, line_recv,
):
    group, slot, level, core, n_levels = position(n_tensor)
    partner = (group, level * 2 + 1 - core)

    def other(k):
        return lax.rem(level + k, n_levels)

    barrier = pltpu.get_barrier_semaphore()
    peers = [(group, other(k) * 2 + core) for k in range(1, n_levels)] + [partner]
    for peer in peers:
        pl.semaphore_signal(barrier, inc=1, device_id=peer, device_id_type=MESH)
    local = []
    for k in range(n_levels):
        copy = pltpu.make_async_copy(part.at[other(k) * 2 + core], mine.at[k], mine_sem.at[k])
        copy.start()
        local.append(copy)
    pl.semaphore_wait(barrier, len(peers))

    pair = []
    for k in [*range(1, n_levels), 0]:
        copy = pltpu.make_async_remote_copy(
            src_ref=part.at[other(k) * 2 + 1 - core], dst_ref=theirs.at[k],
            send_sem=pair_send.at[k], recv_sem=pair_recv.at[k],
            device_id=partner, device_id_type=MESH,
        )
        copy.start()
        pair.append((k, copy))
    for k, copy in pair:
        local[k].wait()
        copy.wait_recv()
        if k > 0:
            summed[k] = (mine[k].astype(jnp.float32) + theirs[k].astype(jnp.float32)).astype(summed.dtype)
    line = []
    for k in range(1, n_levels):
        copy = pltpu.make_async_remote_copy(
            src_ref=summed.at[k], dst_ref=landed.at[k],
            send_sem=line_send.at[k], recv_sem=line_recv.at[k],
            device_id=(group, other(k) * 2 + core), device_id_type=MESH,
        )
        copy.start()
        line.append(copy)
    total = mine[0].astype(jnp.float32) + theirs[0].astype(jnp.float32)
    for k in range(1, n_levels):
        line[k - 1].wait_recv()
        total = total + landed[k].astype(jnp.float32)
    out[...] = total.astype(out.dtype)
    for k, copy in pair:
        copy.wait_send()
    for copy in line:
        copy.wait_send()


def scatter_sum(part, n_tensor):
    rows, width = part.shape[0] // n_tensor, part.shape[1]
    n_levels = n_tensor // 2
    dma = pltpu.SemaphoreType.DMA
    block = pltpu.VMEM((n_levels, rows, width), part.dtype)
    return pl.pallas_call(
        functools.partial(scatter_kernel, n_tensor),
        out_shape=jax.ShapeDtypeStruct((rows, width), part.dtype),
        in_specs=[pl.BlockSpec(memory_space=pl.ANY)],
        out_specs=pl.BlockSpec(memory_space=pltpu.VMEM),
        scratch_shapes=[block] * 4 + [dma((n_levels,))] * 5,
        compiler_params=pltpu.CompilerParams(collective_id=1, has_side_effects=True),
        name="scatter_sum",
    )(part.reshape(n_tensor, rows, width))


def contract(left, right, dims):
    return lax.dot_general(left, right, (dims, ((), ())), preferred_element_type=jnp.float32)


def per_device(n_dp, n_tensor, tokens, out_grad, w_gate, w_up, w_down):
    tok, grad = gather_tokens(tokens, out_grad, n_dp, n_tensor)
    group = lax.axis_index("dp")
    rows, columns = tok.shape[0] // n_dp, tok.shape[1] // n_dp
    gate_val = contract(tok, w_gate, ((1,), (0,)))
    up_val = contract(tok, w_up, ((1,), (0,)))
    grad_hidden = contract(grad, w_down, ((1,), (1,)))
    sigmoid_gate = jax.nn.sigmoid(gate_val)
    act_val = gate_val * sigmoid_gate
    hidden = (act_val * up_val).astype(jnp.bfloat16)
    gate_pre = (
        grad_hidden * up_val * sigmoid_gate * (1.0 + gate_val * (1.0 - sigmoid_gate))
    ).astype(jnp.bfloat16)
    up_pre = (grad_hidden * act_val).astype(jnp.bfloat16)
    hidden, gate_pre, up_pre = lax.optimization_barrier((hidden, gate_pre, up_pre))
    own_gate = lax.dynamic_slice_in_dim(gate_pre, group * rows, rows, 0)
    own_up = lax.dynamic_slice_in_dim(up_pre, group * rows, rows, 0)
    part = (
        contract(own_gate, w_gate, ((1,), (1,))) + contract(own_up, w_up, ((1,), (1,)))
    ).astype(jnp.bfloat16)
    grad_tokens = scatter_sum(part, n_tensor)
    tok_cols = lax.dynamic_slice_in_dim(tok, group * columns, columns, 1)
    grad_cols = lax.dynamic_slice_in_dim(grad, group * columns, columns, 1)
    return (
        grad_tokens,
        contract(tok_cols, gate_pre, ((0,), (0,))).astype(jnp.bfloat16),
        contract(tok_cols, up_pre, ((0,), (0,))).astype(jnp.bfloat16),
        contract(hidden, grad_cols, ((0,), (0,))).astype(jnp.bfloat16),
    )


def solution(mesh):
    n_dp, n_tensor = mesh.shape["dp"], mesh.shape["tensor"]
    in_specs = (
        P(("dp", "tensor"), None),
        P(("dp", "tensor"), None),
        P(None, "tensor"),
        P(None, "tensor"),
        P("tensor", None),
    )
    out_specs = (P(("dp", "tensor"), None), P("dp", "tensor"), P("dp", "tensor"), P("tensor", "dp"))
    return jax.shard_map(
        functools.partial(per_device, n_dp, n_tensor),
        mesh=mesh, in_specs=in_specs, out_specs=out_specs, check_vma=False,
    )
```
